32 devices in a mesh: row: 8 (over z, core), col: 4 (over y, x).
Axes of the slice: x: 2, y: 2, z: 4, core: 2. Of those that a mesh axis runs over, the one named last changes fastest.
Arguments:
- train_weight: bfloat16 [4, 4608, 2048], P(None, 'row', 'col')
- src_map: int32 [16], replicated, may hold values from 0 to 15, as said below
- tgt_map: int32 [16], replicated, may hold values from 0 to 15, as said below
- probe: bfloat16 [4096, 4608], P('row'), may hold values from -6 to 6
Outputs:
- codes: bfloat16 [4, 4608, 2048], P(None, None, 'col')
- peaks: float32 [4, 16], P(None, 'col')
- checked: bfloat16 [4, 4096, 2048], P(None, 'row', 'col')
The draws below stay inside these ranges and needn't reach their ends.
Inputs may be any that keep to these rules, and one draw needn't show every extreme that they name: src_map is a permutation of 0 to 15. tgt_map is a permutation of 0 to 15. Call column k the slots k * 4 to (k + 1) * 4 - 1 of a map, and let C = 4. There are three different offsets a, b, c in 0 to C - 1, the same for every column, of which one is C / 2 and one is C - 1: the heads of training column k stand in serving columns (k - a) mod C (2 of them), (k - b) mod C (one) and (k - c) mod C (one).
All inputs are finite; a program needn't handle non-finite values. Where the reference program divides by a largest or mean magnitude, that divisor is 1e-20 or more.
Results may differ from the reference program's by a relative error of at most 0.0049.
Values may be sent and summed in bfloat16 or wider, within the bound.
No kernel may reach another device: no remote copies, remote signals or barrier semaphores. Data moves between devices by JAX's collectives and lax.ppermute only.
A program may use at most 128 MiB of HBM per device.

```python
import jax
import jax.numpy as jnp

D = 4608
HDIM = 128
HCOL = 4
LAYERS = 4
TOKENS = 4096
N_COL = 4


def head_maps(key):
    heads_all = HCOL * N_COL
    keys = jax.random.split(jax.random.fold_in(key, 17), 6)
    source = jax.random.permutation(keys[0], heads_all).astype(jnp.int32)
    half = N_COL // 2
    before_one = jnp.array([N_COL - 1], jnp.int32)
    picked = jax.random.randint(keys[5], (1,), 0, N_COL - 2).astype(jnp.int32)
    third = jnp.where(picked < half, picked, picked + 1).astype(jnp.int32)
    three = jnp.concatenate([jnp.array([half], jnp.int32), before_one, third])
    offsets = three[jax.random.permutation(keys[4], 3)].astype(jnp.int32)
    pattern = jnp.array([0, 0, 1, 2], jnp.int32)
    roles = jax.vmap(lambda single: jax.random.permutation(single, 4))(jax.random.split(keys[2], N_COL)).astype(jnp.int32)
    locals_order = jax.vmap(lambda single: jax.random.permutation(single, 4))(jax.random.split(keys[3], N_COL)).astype(jnp.int32)
    targets = jnp.arange(N_COL, dtype=jnp.int32)[:, None]
    shifted = offsets[pattern[roles]]
    from_col = (targets + shifted) % N_COL
    local_slot = locals_order[from_col, roles]
    target = source[(from_col * HCOL + local_slot).reshape(-1)]
    return (source, target.astype(jnp.int32))


def draw_src_map(key, part):
    return head_maps(key)[0]


def draw_tgt_map(key, part):
    return head_maps(key)[1]


def draw_train_weight(key, part):
    keys = jax.random.split(jax.random.fold_in(key, 5), 3)
    heads_all = HCOL * N_COL
    head_scale = jnp.exp(jax.random.uniform(keys[1], (LAYERS, 1, heads_all, 1), jnp.float32, jnp.log(0.3), jnp.log(3.0)))
    row_scale = jnp.exp(jax.random.uniform(keys[2], (1, D, 1, 1), jnp.float32, jnp.log(0.4), jnp.log(4.0)))
    base = jax.random.normal(keys[0], (LAYERS, D, heads_all, HDIM), jnp.float32)
    weights = base * head_scale * row_scale / jnp.sqrt(jnp.float32(D))
    return weights.reshape(LAYERS, D, heads_all * HDIM).astype(jnp.bfloat16)


def block_scale(stream_key, shape, cuts, smallest, high):
    def one(position, shards_of):
        heights = jax.random.uniform(jax.random.fold_in(jax.random.fold_in(stream_key, 6), position), (shards_of,), jnp.float32, smallest / len(cuts), high / len(cuts))
        return jnp.repeat(jnp.exp(heights), shape[position] // shards_of).reshape((-1,) + (1,) * (len(shape) - position - 1))

    loudness = one(*cuts[0])
    for cut in cuts[1:]:
        loudness = loudness * one(*cut)
    return loudness


def bell_draw(stream_key, shape, spread, most, cuts=(), kind=jnp.bfloat16):
    loudness = block_scale(stream_key, shape, cuts, -0.22, 0.18) if cuts else 1.0
    entries = jax.random.normal(stream_key, shape, jnp.float32) * spread * loudness
    return jnp.minimum(jnp.maximum(entries, -most), most).astype(kind)


def setup_inputs(seed: int = 0) -> dict:
    streams_of = jax.random.split(jax.random.key(seed), 5)
    return {
        "train_weight": draw_train_weight(jax.random.fold_in(streams_of[4], 71), 0),
        "src_map": draw_src_map(jax.random.fold_in(streams_of[4], 71), 0),
        "tgt_map": draw_tgt_map(jax.random.fold_in(streams_of[4], 71), 0),
        "probe": bell_draw(streams_of[3], (TOKENS, D), 1.0, 6.0, ((0, 8),)),
    }


def reference(train_weight, src_map, tgt_map, probe):
    heads_all = src_map.shape[0]
    slot_ids = jnp.arange(heads_all, dtype=jnp.int32)
    matched = (src_map[None, :] == tgt_map[:, None]).astype(jnp.int32)
    source = jnp.sum(matched * slot_ids[None, :], axis=1).astype(jnp.int32)
    heads_four = train_weight.reshape(LAYERS, D, heads_all, HDIM)
    served = jnp.take(heads_four, source, axis=2)
    peaks = jnp.max(jnp.abs(served.astype(jnp.float32)), axis=(1, 3))
    codes = (served.astype(jnp.float32) / (peaks[:, None, :, None] + 1e-6)).astype(jnp.bfloat16)
    codes = codes.reshape(LAYERS, D, heads_all * HDIM)
    results = []
    for layer in range(LAYERS):
        projected = jnp.dot(probe, codes[layer], preferred_element_type=jnp.float32)
        scaled = projected * jnp.repeat(peaks[layer], HDIM)[None, :]
        results.append(scaled.astype(jnp.bfloat16))
    return codes, peaks, jnp.stack(results)
```

```python
import functools

import jax
import jax.numpy as jnp
from jax import lax
from jax.experimental import pallas as pl
from jax.experimental.pallas import tpu as pltpu
from jax.sharding import PartitionSpec as P

HDIM = 128
CORES = 2
CAP = 2


def routing(src_map, tgt_map, column, col_count, per_col):
    heads = src_map.shape[0]
    ids = jnp.arange(heads, dtype=jnp.int32)
    same = src_map[:, None] == tgt_map[None, :]
    dest = jnp.sum(jnp.where(same, ids[None, :], 0), axis=1)
    origin = jnp.sum(jnp.where(same, ids[:, None], 0), axis=0)
    offset = (ids // per_col - dest // per_col) % col_count
    half, last = col_count // 2, col_count - 1
    kind = jnp.where(offset == half, 0, jnp.where(offset == last, 1, 2))
    third = jnp.max(jnp.where(kind == 2, offset, 0))
    before = (
        (ids[:, None] // per_col == ids[None, :] // per_col)
        & (kind[:, None] == kind[None, :])
        & (ids[None, :] < ids[:, None])
    )
    code = kind * CAP + jnp.sum(before.astype(jnp.int32), axis=1)
    mine = lax.dynamic_slice(code, (column * per_col,), (per_col,))
    wanted = lax.dynamic_slice(origin, (column * per_col,), (per_col,))
    source_code = jnp.sum(jnp.where(wanted[:, None] == ids[None, :], code[None, :], 0), axis=1)
    return mine, wanted, source_code, third


def choose(pieces, flags):
    out = pieces[0]
    for piece, flag in zip(pieces[1:], flags[1:]):
        out = jnp.where(flag, piece, out)
    return out


def heads_of(block, count):
    return [block[:, i * HDIM : (i + 1) * HDIM] for i in range(count)]


def finish_kernel(layer_count, z_count, rows, where_ref, peaks_ref, probe_ref, *refs):
    recv = refs[: 3 * z_count - 1]
    own, rights, lefts = recv[0], recv[1:z_count], recv[z_count : 2 * z_count - 1]
    swapped = recv[2 * z_count - 1 :]
    codes_ref, checked_ref, whole_ref = refs[-3:]
    z, core = where_ref[0], where_ref[1]
    q = pl.program_id(0)
    peaks = peaks_ref[...]
    inverse = 1.0 / ((peaks + 1e-06) * 0.0625)

    def place(block, which):
        start = pl.multiple_of(which * rows, 16)
        scaled = ((block.astype(jnp.float32) * 0.0625) * inverse).astype(jnp.bfloat16)
        codes_ref[0, pl.ds(start, rows), :] = scaled
        begin = pl.multiple_of((q * CORES + which) * rows, 16)
        whole_ref[pl.ds(begin, rows), :] = scaled

    @pl.when(q == z)
    def _():
        place(own[...], core)

    for step in range(1, z_count):

        @pl.when(z - q == step)
        def _():
            place(rights[step - 1][...], core)

        @pl.when(q - z == step)
        def _():
            place(lefts[step - 1][...], core)

    for step in range(z_count):

        @pl.when((z - q == step) | (z - q + z_count == step))
        def _():
            place(swapped[step][...], 1 - core)

    @pl.when(q == z_count - 1)
    def _():
        product = jnp.dot(probe_ref[...], whole_ref[...], preferred_element_type=jnp.float32)
        checked_ref[0] = (product * peaks).astype(jnp.bfloat16)


def finish(layer, layers, z_count, where, peaks, probe, parts, kept):
    rows, width = parts[0].shape
    tokens, depth = probe.shape
    full = lambda shape: pl.BlockSpec(shape, lambda q, w: (0,) * len(shape))
    in_specs = [full((1, width)), full(probe.shape)] + [full((rows, width)) for _ in parts]
    operands = [where, peaks, probe, *parts]
    aliases = {}
    if kept is not None:
        aliases = {len(operands): 0, len(operands) + 1: 1}
        in_specs += [pl.BlockSpec(memory_space=pl.ANY)] * 2
        operands += list(kept)
    return pl.pallas_call(
        functools.partial(finish_kernel, layers, z_count, rows),
        grid_spec=pltpu.PrefetchScalarGridSpec(
            num_scalar_prefetch=1,
            grid=(z_count,),
            in_specs=in_specs,
            out_specs=[
                pl.BlockSpec((1, CORES * rows, width), lambda q, w: (layer, q, 0)),
                pl.BlockSpec((1, tokens, width), lambda q, w: (layer, 0, 0)),
            ],
            scratch_shapes=[pltpu.VMEM((depth, width), jnp.bfloat16)],
        ),
        out_shape=[
            jax.ShapeDtypeStruct((layers, depth, width), jnp.bfloat16),
            jax.ShapeDtypeStruct((layers, tokens, width), jnp.bfloat16),
        ],
        input_output_aliases=aliases,
        compiler_params=pltpu.CompilerParams(
            dimension_semantics=("arbitrary",), vmem_limit_bytes=56 * 1024 * 1024
        ),
        name=f"finish_{layer}",
    )(*operands)


def per_device(train_weight, src_map, tgt_map, probe):
    col_count = lax.axis_size("col")
    row_count = lax.axis_size("row")
    z_count = row_count // CORES
    per_col = src_map.shape[0] // col_count
    layers, rows, width = train_weight.shape
    column = lax.axis_index("col")
    row = lax.axis_index("row")
    z, core = row // CORES, row % CORES
    where = jnp.stack([z, core]).astype(jnp.int32)
    mine, wanted, source_code, third = routing(src_map, tgt_map, column, col_count, per_col)

    def shift(value, by):
        return lax.ppermute(value, "col", [(c, (c - by) % col_count) for c in range(col_count)])

    thirds = [o for o in range(col_count - 1) if o != col_count // 2]

    def exchange(layer):
        pieces = heads_of(train_weight[layer], per_col)
        bufs = [
            jnp.concatenate(
                [
                    choose(pieces, [mine[s] == kind * CAP + rank for s in range(per_col)])
                    for rank in range(CAP)
                ],
                axis=1,
            )
            for kind in range(3)
        ]
        sent = [shift(bufs[0], col_count // 2), shift(bufs[1], col_count - 1)]
        moving = bufs[2]
        for bit in range(max(thirds).bit_length()):
            moved = shift(moving, 1 << bit)
            moving = jnp.where((third >> bit) % 2 == 1, moved, moving)
        sent.append(moving)
        offered = [h for buf in sent for h in heads_of(buf, CAP)]
        return jnp.concatenate(
            [
                choose(offered, [source_code[j] == i for i in range(len(offered))])
                for j in range(per_col)
            ],
            axis=1,
        )

    def along(value, step, direction):
        if direction > 0:
            chips = [(c, c + 1) for c in range(step - 1, z_count - 1)]
        else:
            chips = [(c, c - 1) for c in range(1, z_count - step + 1)]
        pairs = [(a * CORES + k, b * CORES + k) for a, b in chips for k in range(CORES)]
        return lax.ppermute(value, "row", pairs)

    swap_pairs = [(r, r // CORES * CORES + 1 - r % CORES) for r in range(row_count)]

    largest = jnp.max(
        jnp.abs(train_weight.reshape(layers, rows, per_col, HDIM).astype(jnp.float32)), axis=(1, 3)
    )
    everywhere = lax.all_gather(largest, ("row", "col"))
    everywhere = jnp.max(everywhere.reshape(row_count, col_count, layers, per_col), axis=0)
    slots = jnp.transpose(everywhere, (1, 0, 2)).reshape(layers, -1)
    ids = jnp.arange(slots.shape[1], dtype=jnp.int32)
    peaks = jnp.max(
        jnp.where(wanted[None, :, None] == ids[None, None, :], slots[:, None, :], 0.0), axis=2
    )
    lanes = jnp.repeat(peaks, HDIM, axis=1)

    kept = None
    for layer in range(layers):
        own = exchange(layer)
        rights, lefts = [own], [own]
        for step in range(1, z_count):
            rights.append(along(rights[-1], step, 1))
            lefts.append(along(lefts[-1], step, -1))
        swapped = [lax.ppermute(own, "row", swap_pairs)]
        for step in range(1, z_count):
            block = jnp.where(z >= step, rights[step], lefts[z_count - step])
            swapped.append(lax.ppermute(block, "row", swap_pairs))
        parts = [own, *rights[1:], *lefts[1:], *swapped]
        kept = finish(layer, layers, z_count, where, lanes[layer : layer + 1], probe, parts, kept)
    codes, checked = kept
    return (codes, peaks, checked)


def solution(mesh):
    in_specs = (P(None, "row", "col"), P(), P(), P("row", None))
    out_specs = (P(None, None, "col"), P(None, "col"), P(None, "row", "col"))
    return jax.shard_map(
        per_device, mesh=mesh, in_specs=in_specs, out_specs=out_specs, check_vma=False
    )
```

```python
import functools

import jax
import jax.numpy as jnp
from jax import lax
from jax.experimental import pallas as pl
from jax.experimental.pallas import tpu as pltpu
from jax.sharding import PartitionSpec as P

HDIM = 128
CAP = 2


def find(table, value, size):
    return lax.fori_loop(
        0, size, lambda i, at: jnp.where(table[i] == value, i, at), jnp.int32(0)
    )


def kind_of(offset, col_count):
    return jnp.where(offset == col_count // 2, 0, jnp.where(offset == col_count - 1, 1, 2))


def pack_kernel(col_count, per_col, column_ref, src_ref, tgt_ref, weight_ref, *bufs):
    column = column_ref[0]
    kinds = []
    for slot in range(per_col):
        dest = find(tgt_ref, src_ref[column * per_col + slot], col_count * per_col)
        offset = lax.rem(column - lax.div(dest, per_col) + col_count, col_count)
        kinds.append(kind_of(offset, col_count))
    for slot in range(per_col):
        rank = sum([(kinds[s] == kinds[slot]).astype(jnp.int32) for s in range(slot)], jnp.int32(0))
        code = kinds[slot] * CAP + rank
        for place in range(3 * CAP):

            @pl.when(code == place)
            def _():
                lane = (place % CAP) * HDIM
                bufs[place // CAP][:, :, lane : lane + HDIM] = weight_ref[
                    :, :, slot * HDIM : (slot + 1) * HDIM
                ]


def unpack_kernel(col_count, per_col, bit, column_ref, src_ref, tgt_ref, *refs):
    column = column_ref[0]
    half_ref, last_ref, stay_ref, moved_ref, own_ref = refs
    heads = col_count * per_col
    found = [find(src_ref, tgt_ref[column * per_col + j], heads) for j in range(per_col)]
    for j in range(per_col):
        origin = lax.div(found[j], per_col)
        offset = lax.rem(origin - column + col_count, col_count)
        kind = kind_of(offset, col_count)
        kind = jnp.where((kind == 2) & (lax.rem(lax.shift_right_logical(offset, bit), 2) == 1), 3, kind)
        rank = sum(
            [
                ((lax.div(f, per_col) == origin) & (f < found[j])).astype(jnp.int32)
                for f in found
            ],
            jnp.int32(0),
        )
        code = kind * CAP + rank
        for place in range(4 * CAP):

            @pl.when(code == place)
            def _():
                lane = (place % CAP) * HDIM
                source = (half_ref, last_ref, stay_ref, moved_ref)[place // CAP]
                own_ref[:, :, j * HDIM : (j + 1) * HDIM] = source[:, :, lane : lane + HDIM]


def on_blocks(body, maps, operands, out_widths, name):
    layers, rows, _ = operands[0].shape
    spec = lambda width: pl.BlockSpec((1, rows, width), lambda l, *_: (l, 0, 0))
    return pl.pallas_call(
        body,
        grid_spec=pltpu.PrefetchScalarGridSpec(
            num_scalar_prefetch=len(maps),
            grid=(layers,),
            in_specs=[spec(o.shape[2]) for o in operands],
            out_specs=[spec(w) for w in out_widths],
        ),
        out_shape=[jax.ShapeDtypeStruct((layers, rows, w), jnp.bfloat16) for w in out_widths],
        compiler_params=pltpu.CompilerParams(dimension_semantics=("arbitrary",)),
        name=name,
    )(*maps, *operands)


def finish_kernel(tiles, tile, x_ref, probe_ref, *refs):
    codes_ref, checked_ref, peaks_ref, whole_ref, top_ref, sum_ref = refs[-6:]
    i = pl.program_id(0)
    width = top_ref.shape[1]

    @pl.when(i < tiles)
    def _():
        x = x_ref[...]
        whole_ref[pl.ds(pl.multiple_of(i * tile, tile), tile), :] = x
        here = jnp.max(jnp.abs(x.astype(jnp.float32)), axis=0, keepdims=True)
        top_ref[...] = jnp.where(i == 0, here, jnp.maximum(top_ref[...], here))

    @pl.when(i == tiles - 1)
    def _():
        for head in range(width // HDIM):
            lanes = slice(head * HDIM, (head + 1) * HDIM)
            top = jnp.max(top_ref[:, lanes], axis=1, keepdims=True)
            peaks_ref[:, lanes] = jnp.broadcast_to(top, (1, HDIM))

    @pl.when(i >= tiles)
    def _():
        k = i - tiles
        inverse = 1.0 / ((peaks_ref[...] + 1e-06) * 0.0625)
        x = whole_ref[pl.ds(pl.multiple_of(k * tile, tile), tile), :]
        codes = ((x.astype(jnp.float32) * 0.0625) * inverse).astype(jnp.bfloat16)
        codes_ref[0] = codes
        part = jnp.dot(probe_ref[...], codes, preferred_element_type=jnp.float32)

        @pl.when(k == 0)
        def _():
            sum_ref[...] = part

        @pl.when(k > 0)
        def _():
            sum_ref[...] += part

        @pl.when(k == tiles - 1)
        def _():
            checked_ref[0] = (sum_ref[...] * peaks_ref[...]).astype(jnp.bfloat16)


def finish(layer, layers, joined, probe, kept):
    depth, width = joined.shape
    tokens = probe.shape[0]
    tile = max(t for t in range(128, 1153, 128) if depth % t == 0)
    tiles = depth // tile
    in_specs = [
        pl.BlockSpec((tile, width), lambda i: (jnp.minimum(i, tiles - 1), 0)),
        pl.BlockSpec((tokens, tile), lambda i: (0, jnp.maximum(i - tiles, 0))),
    ]
    operands = [joined, probe]
    aliases = {}
    if kept is not None:
        aliases = {2: 0, 3: 1}
        in_specs += [pl.BlockSpec(memory_space=pl.ANY)] * 2
        operands += list(kept)
    codes, checked, peaks = pl.pallas_call(
        functools.partial(finish_kernel, tiles, tile),
        grid=(2 * tiles,),
        in_specs=in_specs,
        out_specs=[
            pl.BlockSpec((1, tile, width), lambda i: (layer, jnp.maximum(i - tiles, 0), 0)),
            pl.BlockSpec((1, tokens, width), lambda i: (layer, 0, 0)),
            pl.BlockSpec((1, width), lambda i: (0, 0)),
        ],
        out_shape=[
            jax.ShapeDtypeStruct((layers, depth, width), jnp.bfloat16),
            jax.ShapeDtypeStruct((layers, tokens, width), jnp.bfloat16),
            jax.ShapeDtypeStruct((1, width), jnp.float32),
        ],
        scratch_shapes=[
            pltpu.VMEM((depth, width), jnp.bfloat16),
            pltpu.VMEM((1, width), jnp.float32),
            pltpu.VMEM((tokens, width), jnp.float32),
        ],
        input_output_aliases=aliases,
        compiler_params=pltpu.CompilerParams(
            dimension_semantics=("arbitrary",), vmem_limit_bytes=40 * 1024 * 1024
        ),
        name=f"finish_{layer}",
    )(*operands)
    return (codes, checked), peaks


def third_offset(src_map, tgt_map, col_count, per_col):
    heads = src_map.shape[0]
    ids = jnp.arange(heads, dtype=jnp.int32)
    same = src_map[:per_col, None] == tgt_map[None, :]
    dest = jnp.sum(jnp.where(same, ids[None, :], 0), axis=1)
    offset = (-(dest // per_col)) % col_count
    known = (offset == col_count // 2) | (offset == col_count - 1)
    return jnp.max(jnp.where(known, 0, offset))


def per_device(train_weight, src_map, tgt_map, probe):
    col_count = lax.axis_size("col")
    per_col = src_map.shape[0] // col_count
    layers, rows, width = train_weight.shape
    maps = [lax.axis_index("col").reshape(1).astype(jnp.int32), src_map, tgt_map]
    bits = max(o for o in range(col_count - 1) if o != col_count // 2).bit_length()
    third = third_offset(src_map, tgt_map, col_count, per_col) if bits > 1 else None

    def shift(value, by):
        return lax.ppermute(value, "col", [(c, (c - by) % col_count) for c in range(col_count)])

    def exchange(block, name):
        half, last, moving = on_blocks(
            functools.partial(pack_kernel, col_count, per_col),
            maps, [block], [CAP * HDIM] * 3, f"pack_{name}",
        )
        half, last = shift(half, col_count // 2), shift(last, col_count - 1)
        for bit in range(bits - 1):
            moving = jnp.where((third >> bit) % 2 == 1, shift(moving, 1 << bit), moving)
        moved = shift(moving, 1 << (bits - 1))
        return on_blocks(
            functools.partial(unpack_kernel, col_count, per_col, bits - 1),
            maps, [half, last, moving, moved], [width], f"unpack_{name}",
        )[0]

    own = [exchange(train_weight[:1], "first")]
    rest, own[0] = lax.optimization_barrier((train_weight[1:], own[0]))
    own.append(exchange(rest, "rest"))
    kept, peaks = None, []
    for layer in range(layers):
        block = own[0][0] if layer == 0 else own[1][layer - 1]
        joined = lax.all_gather(block, "row", axis=0, tiled=True)
        kept, top = finish(layer, layers, joined, probe, kept)
        peaks.append(top)
    codes, checked = kept
    peaks = jnp.concatenate(peaks, axis=0).reshape(layers, per_col, HDIM)[:, :, 0]
    return (codes, peaks, checked)


def solution(mesh):
    in_specs = (P(None, "row", "col"), P(), P(), P("row", None))
    out_specs = (P(None, None, "col"), P(None, "col"), P(None, "row", "col"))
    return jax.shard_map(
        per_device, mesh=mesh, in_specs=in_specs, out_specs=out_specs, check_vma=False
    )
```

```python
import functools

import jax
import jax.numpy as jnp
from jax import lax
from jax.experimental import pallas as pl
from jax.experimental.pallas import tpu as pltpu
from jax.sharding import PartitionSpec as P

HDIM = 128
CAP = 2

GRANT = 60 * 1024 * 1024


def find(table, value, size):
    return lax.fori_loop(
        0, size, lambda i, at: jnp.where(table[i] == value, i, at), jnp.int32(0)
    )


def kind_of(offset, col_count):
    return jnp.where(offset == col_count // 2, 0, jnp.where(offset == col_count - 1, 1, 2))


def pack_kernel(col_count, per_col, column_ref, src_ref, tgt_ref, weight_ref, *bufs):
    column = column_ref[0]
    kinds = []
    for slot in range(per_col):
        dest = find(tgt_ref, src_ref[column * per_col + slot], col_count * per_col)
        offset = lax.rem(column - lax.div(dest, per_col) + col_count, col_count)
        kinds.append(kind_of(offset, col_count))
    for slot in range(per_col):
        rank = sum([(kinds[s] == kinds[slot]).astype(jnp.int32) for s in range(slot)], jnp.int32(0))
        code = kinds[slot] * CAP + rank
        for place in range(3 * CAP):

            @pl.when(code == place)
            def _():
                lane = (place % CAP) * HDIM
                bufs[place // CAP][:, :, lane : lane + HDIM] = weight_ref[
                    :, :, slot * HDIM : (slot + 1) * HDIM
                ]


def unpack_kernel(col_count, per_col, bit, column_ref, src_ref, tgt_ref, *refs):
    column = column_ref[0]
    half_ref, last_ref, stay_ref, moved_ref, own_ref = refs
    heads = col_count * per_col
    found = [find(src_ref, tgt_ref[column * per_col + j], heads) for j in range(per_col)]
    for j in range(per_col):
        origin = lax.div(found[j], per_col)
        offset = lax.rem(origin - column + col_count, col_count)
        kind = kind_of(offset, col_count)
        kind = jnp.where((kind == 2) & (lax.rem(lax.shift_right_logical(offset, bit), 2) == 1), 3, kind)
        rank = sum(
            [
                ((lax.div(f, per_col) == origin) & (f < found[j])).astype(jnp.int32)
                for f in found
            ],
            jnp.int32(0),
        )
        code = kind * CAP + rank
        for place in range(4 * CAP):

            @pl.when(code == place)
            def _():
                lane = (place % CAP) * HDIM
                source = (half_ref, last_ref, stay_ref, moved_ref)[place // CAP]
                own_ref[:, :, j * HDIM : (j + 1) * HDIM] = source[:, :, lane : lane + HDIM]


def on_blocks(body, maps, operands, out_widths, name, first, layers):
    rows = operands[0].shape[1]
    spec = lambda width, at=0: pl.BlockSpec((1, rows, width), lambda l, *_: (l + at, 0, 0))
    return pl.pallas_call(
        body,
        grid_spec=pltpu.PrefetchScalarGridSpec(
            num_scalar_prefetch=len(maps),
            grid=(layers,),
            in_specs=[spec(o.shape[2], first) for o in operands],
            out_specs=[spec(w) for w in out_widths],
        ),
        out_shape=[jax.ShapeDtypeStruct((layers, rows, w), jnp.bfloat16) for w in out_widths],
        compiler_params=pltpu.CompilerParams(
            dimension_semantics=("arbitrary",), vmem_limit_bytes=GRANT
        ),
        name=name,
    )(*maps, *operands)


def finish_kernel(tiles, tile, x_ref, probe_ref, *refs):
    codes_ref, checked_ref, peaks_ref, whole_ref, top_ref, sum_ref = refs[-6:]
    i = pl.program_id(0)
    width = top_ref.shape[1]

    @pl.when(i < tiles)
    def _():
        x = x_ref[0]
        whole_ref[pl.ds(pl.multiple_of(i * tile, tile), tile), :] = x
        here = jnp.max(jnp.abs(x.astype(jnp.float32)), axis=0, keepdims=True)
        top_ref[...] = jnp.where(i == 0, here, jnp.maximum(top_ref[...], here))

    @pl.when(i == tiles - 1)
    def _():
        for head in range(width // HDIM):
            lanes = slice(head * HDIM, (head + 1) * HDIM)
            top = jnp.max(top_ref[:, lanes], axis=1, keepdims=True)
            peaks_ref[:, lanes] = jnp.broadcast_to(top, (1, HDIM))

    @pl.when(i >= tiles)
    def _():
        k = i - tiles
        inverse = 1.0 / ((peaks_ref[...] + 1e-06) * 0.0625)
        x = whole_ref[pl.ds(pl.multiple_of(k * tile, tile), tile), :]
        codes = ((x.astype(jnp.float32) * 0.0625) * inverse).astype(jnp.bfloat16)
        codes_ref[0] = codes
        part = jnp.dot(probe_ref[...], codes, preferred_element_type=jnp.float32)

        @pl.when(k == 0)
        def _():
            sum_ref[...] = part

        @pl.when(k > 0)
        def _():
            sum_ref[...] += part

        @pl.when(k == tiles - 1)
        def _():
            checked_ref[0] = (sum_ref[...] * peaks_ref[...]).astype(jnp.bfloat16)


def finish(layer, part, layers, joined, probe, kept):
    _, depth, width = joined.shape
    tokens = probe.shape[0]
    tile = max(t for t in range(128, 1153, 128) if depth % t == 0)
    tiles = depth // tile
    in_specs = [
        pl.BlockSpec((1, tile, width), lambda i: (part, jnp.minimum(i, tiles - 1), 0)),
        pl.BlockSpec((tokens, tile), lambda i: (0, jnp.maximum(i - tiles, 0))),
    ]
    operands = [joined, probe]
    aliases = {}
    if kept is not None:
        aliases = {2: 0, 3: 1}
        in_specs += [pl.BlockSpec(memory_space=pl.ANY)] * 2
        operands += list(kept)
    codes, checked, peaks = pl.pallas_call(
        functools.partial(finish_kernel, tiles, tile),
        grid=(2 * tiles,),
        in_specs=in_specs,
        out_specs=[
            pl.BlockSpec((1, tile, width), lambda i: (layer, jnp.maximum(i - tiles, 0), 0)),
            pl.BlockSpec((1, tokens, width), lambda i: (layer, 0, 0)),
            pl.BlockSpec((1, width), lambda i: (0, 0)),
        ],
        out_shape=[
            jax.ShapeDtypeStruct((layers, depth, width), jnp.bfloat16),
            jax.ShapeDtypeStruct((layers, tokens, width), jnp.bfloat16),
            jax.ShapeDtypeStruct((1, width), jnp.float32),
        ],
        scratch_shapes=[
            pltpu.VMEM((depth, width), jnp.bfloat16),
            pltpu.VMEM((1, width), jnp.float32),
            pltpu.VMEM((tokens, width), jnp.float32),
        ],
        input_output_aliases=aliases,
        compiler_params=pltpu.CompilerParams(
            dimension_semantics=("arbitrary",), vmem_limit_bytes=GRANT
        ),
        name=f"finish_{layer}",
    )(*operands)
    return (codes, checked), peaks


def third_offset(src_map, tgt_map, col_count, per_col):
    heads = src_map.shape[0]
    ids = jnp.arange(heads, dtype=jnp.int32)
    same = src_map[:per_col, None] == tgt_map[None, :]
    dest = jnp.sum(jnp.where(same, ids[None, :], 0), axis=1)
    offset = (-(dest // per_col)) % col_count
    known = (offset == col_count // 2) | (offset == col_count - 1)
    return jnp.max(jnp.where(known, 0, offset))


def per_device(train_weight, src_map, tgt_map, probe):
    col_count = lax.axis_size("col")
    per_col = src_map.shape[0] // col_count
    layers, rows, width = train_weight.shape
    maps = [lax.axis_index("col").reshape(1).astype(jnp.int32), src_map, tgt_map]
    bits = max(o for o in range(col_count - 1) if o != col_count // 2).bit_length()
    third = third_offset(src_map, tgt_map, col_count, per_col) if bits > 1 else None

    def shift(value, by):
        return lax.ppermute(value, "col", [(c, (c - by) % col_count) for c in range(col_count)])

    def exchange(weight, first, count):
        half, last, moving = on_blocks(
            functools.partial(pack_kernel, col_count, per_col),
            maps, [weight], [CAP * HDIM] * 3, f"pack_{first}", first, count,
        )
        half, last = shift(half, col_count // 2), shift(last, col_count - 1)
        for bit in range(bits - 1):
            moving = jnp.where((third >> bit) % 2 == 1, shift(moving, 1 << bit), moving)
        moved = shift(moving, 1 << (bits - 1))
        return on_blocks(
            functools.partial(unpack_kernel, col_count, per_col, bits - 1),
            maps, [half, last, moving, moved], [width], f"unpack_{first}", 0, count,
        )[0]

    groups = [(0, 1), (1, layers - 2), (layers - 1, 1)]
    own, weight = [], train_weight
    for first, count in groups:
        block = exchange(weight, first, count)
        weight, block = lax.optimization_barrier((weight, block))
        own.append(block)
    kept, peaks = None, []
    for (first, count), block in zip(groups, own):
        joined = lax.all_gather(block, "row", axis=1, tiled=True)
        for part in range(count):
            kept, top = finish(first + part, part, layers, joined, probe, kept)
            peaks.append(top)
    codes, checked = kept
    peaks = jnp.concatenate(peaks, axis=0).reshape(layers, per_col, HDIM)[:, :, 0]
    return (codes, peaks, checked)


def solution(mesh):
    in_specs = (P(None, "row", "col"), P(), P(), P("row", None))
    out_specs = (P(None, None, "col"), P(None, "col"), P(None, "row", "col"))
    return jax.shard_map(
        per_device, mesh=mesh, in_specs=in_specs, out_specs=out_specs, check_vma=False
    )
```
